32 devices in a mesh: group: 2 (over x), tile: 16 (over z, y, core).
Axes of the slice: x: 2, y: 2, z: 4, core: 2. Of those that a mesh axis runs over, the one named last changes fastest.
Arguments:
- hadamard: int32 [128, 1152], P(None, 'tile'), may hold values from -1 to 1, as said below
- stroke: float32 [2304], P(('group', 'tile')), parts along dimension 0, may hold values from 0.3 to 1
- influence: bfloat16 [3, 2304, 8192], P(None, ('group', 'tile')), parts along dimension 1, may hold values from -0.4375 to 0.4375
- amplitude: float32 [1024, 16, 16], P(('group', 'tile')), parts along dimension 0, may hold values from 0.3 to 1
- aberration: float32 [1024, 16, 16], P(('group', 'tile')), parts along dimension 0, may hold values from -3 to 3
- valid_mask: int32 [1024], P(('group', 'tile')), parts along dimension 0, may hold values from 0 to 1, as said below
Outputs:
- imat: float32 [2304, 2, 512], P(('group', 'tile')), parts along dimension 0
The draws below stay inside these ranges and needn't reach their ends.
There are 2 independent parts, one for each index of `group`. The reference program is written for one: setup_inputs(seed, part) draws one part's arguments, and reference() takes and returns one part's arrays. A program takes and returns all parts, laid end to end along the dimension named above; an argument that names none is the same for every part. Nothing has to cross between parts.
Inputs may be any that keep to these rules, and one draw needn't show every extreme that they name: `hadamard`: each column is one column of a Sylvester-Hadamard matrix whose order is the least power of two not below 1152, restricted to 128 distinct rows of it; different actuators take different columns. `valid_mask`: every pupil tile of 32 subapertures holds at least one valid subaperture.
All inputs are finite; a program needn't handle non-finite values.
Results may differ from the reference program's by a relative error of at most 0.0055.
Values may be sent and summed in bfloat16 or wider, within the bound.
A program may use at most 128 MiB of HBM per device.

```python
import math
import jax
import jax.numpy as jnp
from jax import lax

PAT = 128
ACT_DEV = 72
SUB_DEV = 32
SAMP = 16
PIX = 16
ACTS = 1152
SUBS = 512
PTS = 8192
N_TILE = 16


def draw_hadamard(key, part):
    order_bits = max(1, (ACTS - 1).bit_length())
    order = 2 ** order_bits
    row_pick = jax.random.permutation(jax.random.fold_in(key, 17), order)[:PAT].astype(jnp.int32)
    column_pick = jax.random.permutation(jax.random.fold_in(key, 29), order)[:ACTS].astype(jnp.int32)
    shared = jnp.bitwise_and(row_pick[:, None], column_pick[None, :])
    parity = jnp.zeros((PAT, ACTS), jnp.int32)
    for place in range(order_bits):
        parity = jnp.bitwise_xor(parity, jnp.bitwise_and(jnp.right_shift(shared, place), 1))
    return (1 - 2 * parity).astype(jnp.int32)


def draw_valid_mask(key, part):
    base_draw = jax.random.randint(jax.random.fold_in(key, 41), (N_TILE, SUB_DEV), 0, 4)
    base_mask = (base_draw < 3).astype(jnp.int32)
    forced_place = jax.random.randint(jax.random.fold_in(key, 53), (N_TILE, 1), 0, SUB_DEV)
    places = jnp.arange(SUB_DEV, dtype=jnp.int32)[None, :]
    forced = (places == forced_place).astype(jnp.int32)
    return jnp.maximum(base_mask, forced).reshape(SUBS).astype(jnp.int32)


def block_scale(stream_key, extent, shards, low, largest):
    factor_of, own = 1.0, jax.random.fold_in(stream_key, 6)
    for axis_at, shards_of in shards:
        draws = jnp.exp(jax.random.uniform(jax.random.fold_in(own, axis_at), (shards_of,), jnp.float32, low / len(shards), largest / len(shards)))
        factor_of = factor_of * jnp.repeat(draws, extent[axis_at] // shards_of).reshape([-1 if axis == axis_at else 1 for axis in range(len(extent))])
    return factor_of


def normal_values(own_key, dims, width, most, pieces=(), kind=jnp.bfloat16):
    level = block_scale(own_key, dims, pieces, -0.22, 0.18) if pieces else 1.0
    drawn = jax.random.normal(own_key, dims, jnp.float32) * width * level
    return jnp.minimum(jnp.maximum(drawn, -most), most).astype(kind)


def setup_inputs(seed: int = 0, part: int = 0) -> dict:
    splits = jax.random.split(jax.random.key(seed), 7)
    own_keys = jax.random.split(jax.random.fold_in(splits[6], part), 7)
    return {
        "hadamard": draw_hadamard(jax.random.fold_in(splits[6], 71), part),
        "stroke": jnp.clip(jnp.exp(math.log(1.0) - 1.2039728 * jax.random.uniform(own_keys[1], (ACTS,), jnp.float32) ** block_scale(own_keys[1], (ACTS,), ((0, 16),), -0.2, 0.2)), 0.3, 1.0),
        "influence": normal_values(own_keys[2], (3, ACTS, PTS), (3 * ACT_DEV) ** -0.5, 0.4375, ((1, 16),)),
        "amplitude": jnp.clip(jnp.exp(math.log(1.0) - 1.2039728 * jax.random.uniform(own_keys[3], (SUBS, SAMP, SAMP), jnp.float32) ** block_scale(own_keys[3], (SUBS, SAMP, SAMP), ((0, 16),), -0.2, 0.2)), 0.3, 1.0),
        "aberration": normal_values(own_keys[4], (SUBS, SAMP, SAMP), 0.5, 3.0, ((0, 16),), jnp.float32),
        "valid_mask": draw_valid_mask(jax.random.fold_in(jax.random.fold_in(splits[6], part), 71), part),
    }


HIGHEST = lax.Precision.HIGHEST


def transform_tables(samples, pixels):
    freqs = jnp.arange(pixels, dtype=jnp.float32) - pixels / 2.0
    places = jnp.arange(samples, dtype=jnp.float32)
    angle = 2.0 * jnp.pi * freqs[:, None] * places[None, :] / (2.0 * samples)
    return jnp.cos(angle), -jnp.sin(angle)


def kron_tables(samples, pixels):
    table_real, table_imag = transform_tables(samples, pixels)
    kron_real = jnp.kron(table_real, table_real) - jnp.kron(table_imag, table_imag)
    kron_imag = jnp.kron(table_real, table_imag) + jnp.kron(table_imag, table_real)
    upper = jnp.concatenate([kron_real.T, kron_imag.T], axis=1)
    lower = jnp.concatenate([-kron_imag.T, kron_real.T], axis=1)
    transform = jnp.concatenate([upper, lower], axis=0)
    centre = jnp.arange(pixels, dtype=jnp.float32) - (pixels - 1) / 2.0
    along_u = jnp.repeat(centre, pixels)
    along_v = jnp.tile(centre, pixels)
    moments = jnp.stack([jnp.ones_like(along_u), along_u, along_v], axis=1)
    return transform, moments


def spot_slopes(phase_map, amplitude, aberration, valid_mask):
    patterns, sub_count, samples = phase_map.shape[0], phase_map.shape[1], phase_map.shape[2]
    flat = samples * samples
    transform, moments = kron_tables(samples, PIX)
    half = PIX * PIX
    phase_rows = phase_map.reshape(patterns, sub_count, flat)
    amp_rows = amplitude.reshape(sub_count, flat)[None]
    abe_rows = aberration.reshape(sub_count, flat)[None]
    results = []
    for pattern_sign in (1.0, -1.0):
        angles = abe_rows + pattern_sign * phase_rows
        field = jnp.concatenate([amp_rows * jnp.cos(angles), amp_rows * jnp.sin(angles)], axis=2)
        focal = jnp.dot(field.reshape(patterns * sub_count, 2 * flat), transform, precision=HIGHEST)
        intensity = focal[:, :half] * focal[:, :half] + focal[:, half:] * focal[:, half:]
        sums = jnp.dot(intensity, moments, precision=HIGHEST)
        centroid_x = sums[:, 1] / sums[:, 0]
        centroid_y = sums[:, 2] / sums[:, 0]
        results.append(jnp.stack([centroid_x, centroid_y], axis=1).reshape(patterns, sub_count, 2).transpose(0, 2, 1))
    weights = valid_mask.astype(jnp.float32)[None, None, :]
    return ((results[0] - results[1]) * 0.5 * weights).astype(jnp.bfloat16)


def reference(hadamard, stroke, influence, amplitude, aberration, valid_mask):
    commands = (stroke[None, :] * hadamard.astype(jnp.float32)).astype(jnp.bfloat16)

    def one_tile(tile_index):
        phase_map = jnp.zeros((PAT, PTS), jnp.float32)
        for offset in range(3):
            source = tile_index + 1 - offset
            inside = (source >= 0) & (source < N_TILE)
            clipped = jnp.clip(source, 0, N_TILE - 1).astype(jnp.int32)
            block_cmds = lax.dynamic_slice_in_dim(commands, clipped * ACT_DEV, ACT_DEV, 1)
            block_infl = lax.dynamic_slice_in_dim(influence[offset], clipped * ACT_DEV, ACT_DEV, 0)
            term = jnp.dot(block_cmds, block_infl, preferred_element_type=jnp.float32).astype(jnp.bfloat16)
            term = lax.optimization_barrier(term).astype(jnp.float32)
            phase_map = phase_map + jnp.where(inside, term, jnp.zeros_like(term))
        first = (tile_index * SUB_DEV).astype(jnp.int32)
        amp_tile = lax.dynamic_slice_in_dim(amplitude, first, SUB_DEV, 0)
        abe_tile = lax.dynamic_slice_in_dim(aberration, first, SUB_DEV, 0)
        mask_tile = lax.dynamic_slice_in_dim(valid_mask, first, SUB_DEV, 0)
        return spot_slopes(phase_map.reshape(PAT, SUB_DEV, SAMP, SAMP), amp_tile, abe_tile, mask_tile)

    per_tile = lax.map(one_tile, jnp.arange(N_TILE, dtype=jnp.int32))
    slopes = jnp.transpose(per_tile, (1, 2, 0, 3)).reshape(PAT, 2 * SUBS)
    summed = jnp.dot(hadamard.astype(jnp.bfloat16).T, slopes, preferred_element_type=jnp.float32)
    return summed.reshape(ACTS, 2, SUBS) / (PAT * stroke)[:, None, None]
```

```python
import functools
import math

import jax
import jax.numpy as jnp
import numpy as np
from jax import lax
from jax.experimental import pallas as pl
from jax.experimental.pallas import tpu as pltpu
from jax.sharding import PartitionSpec as P

PIX = 16
MESH = pl.DeviceIdType.MESH
NT = (((1,), (1,)), ((), ()))


def dft_table(samples, pixels):
    freqs = np.arange(pixels) - pixels / 2.0
    wave = np.exp(-2j * np.pi * freqs[:, None] * np.arange(samples)[None, :] / (2.0 * samples))
    kron = np.kron(wave, wave)
    return np.block([[kron.real, -kron.imag], [kron.imag, kron.real]]).astype(np.float32)


def poly_fit(func, degree):
    fit = np.polynomial.chebyshev.Chebyshev.interpolate(func, degree, domain=[0.0, 0.25])
    return [float(c) for c in fit.convert(kind=np.polynomial.Polynomial).coef]


def sin_over_r(z):
    return 2 * np.pi * np.sinc(2 * np.sqrt(z))


COS = poly_fit(lambda z: np.cos(2 * np.pi * np.sqrt(z)), 5)
SIN = poly_fit(sin_over_r, 5)


def horner(coefs, z):
    total = coefs[-1] * z + coefs[-2]
    for c in coefs[-3::-1]:
        total = total * z + c
    return total


def cos_sin(phase):
    turns = phase * (1.0 / (2.0 * math.pi))
    r = turns - jnp.round(turns)
    z = r * r
    return horner(COS, z), r * horner(SIN, z)


def column_sums(planes):
    pix = len(planes)
    run = planes[-1]
    nested = run
    for plane in planes[-2::-1]:
        run = run + plane
        nested = nested + run
    places = lax.broadcasted_iota(jnp.int32, run.shape, 0).astype(jnp.float32)
    centre = (pix - 1) / 2.0
    along_u = nested - (centre + 1.0) * run
    along_v = run * (places - centre)
    return [jnp.sum(x, axis=0, keepdims=True) for x in (run, along_u, along_v)]


def spot_rows(phase, real, imag, table):
    patterns = phase.shape[0]
    cs, sn = cos_sin(phase)
    even = jnp.concatenate([(cs * real).astype(jnp.bfloat16), (cs * imag).astype(jnp.bfloat16)], axis=1)
    odd = jnp.concatenate([(sn * -imag).astype(jnp.bfloat16), (sn * real).astype(jnp.bfloat16)], axis=1)
    field = jnp.concatenate([even, odd], axis=0)
    focal = lax.dot_general(table, field, NT, preferred_element_type=jnp.float32)
    half = focal.shape[0] // 2
    squares, crosses = [], []
    for u in range(PIX):
        re = focal[u * PIX:(u + 1) * PIX]
        im = focal[half + u * PIX:half + (u + 1) * PIX]
        c_re, s_re = re[:, :patterns], re[:, patterns:]
        c_im, s_im = im[:, :patterns], im[:, patterns:]
        squares.append((c_re * c_re + c_im * c_im) + (s_re * s_re + s_im * s_im))
        crosses.append(c_re * s_re + c_im * s_im)
    p0, pu, pv = column_sums(squares)
    q0, qu, qv = [2.0 * x for x in column_sums(crosses)]
    scale = 1.0 / ((p0 + q0) * (p0 - q0))
    return (qu * p0 - pu * q0) * scale, (qv * p0 - pv * q0) * scale


def slopes_kernel(per_step, flat, cmd_ref, mid_ref, low_ref, up_ref, real_ref, imag_ref, mask_ref, table_ref, out_ref):
    rows_u, rows_v = [], []
    for k in range(per_step):
        cols = pl.ds(k * flat, flat)
        phase = jnp.dot(cmd_ref[0], low_ref[:, cols], preferred_element_type=jnp.float32)
        phase += jnp.dot(cmd_ref[1], mid_ref[0, :, cols], preferred_element_type=jnp.float32)
        phase += jnp.dot(cmd_ref[2], up_ref[:, cols], preferred_element_type=jnp.float32)
        along_u, along_v = spot_rows(phase, real_ref[k:k + 1, :], imag_ref[k:k + 1, :], table_ref[...])
        rows_u.append(along_u)
        rows_v.append(along_v)
    mask = mask_ref[...]
    out_ref[0] = (jnp.concatenate(rows_u, axis=0) * mask).astype(out_ref.dtype)
    out_ref[1] = (jnp.concatenate(rows_v, axis=0) * mask).astype(out_ref.dtype)


def gather_kernel(n, mine_ref, had_ref, out_ref, held, own_sem, send_sems, recv_sems):
    me = lax.axis_index("tile")
    subs = mine_ref.shape[1]
    barrier = pltpu.get_barrier_semaphore()

    @pl.loop(1, n)
    def _(k):
        pl.semaphore_signal(barrier, inc=1, device_id={"tile": lax.rem(me + k, n)}, device_id_type=MESH)

    pl.semaphore_wait(barrier, n - 1)
    slot = held.at[:, pl.ds(pl.multiple_of(me * subs, subs), subs), :]
    own = pltpu.make_async_copy(mine_ref, slot, own_sem)
    own.start()

    def push(k):
        return pltpu.make_async_remote_copy(
            src_ref=mine_ref,
            dst_ref=slot,
            send_sem=send_sems.at[k],
            recv_sem=recv_sems.at[k],
            device_id={"tile": lax.rem(me + k, n)},
            device_id_type=MESH,
        )

    @pl.loop(1, n)
    def _(k):
        push(k).start()

    own.wait()

    @pl.loop(1, n)
    def _(k):
        push(k).wait()

    for c in range(2):
        out_ref[c] = lax.dot_general(had_ref[...], held[c], NT, preferred_element_type=jnp.float32)


def passed_along(value, axis, steps):
    count = lax.axis_size(axis)
    first, last = (max(0, -steps), min(count, count - steps))
    return lax.ppermute(value, axis, [(source, source + steps) for source in range(first, last)])


def per_device(hadamard, stroke, influence, amplitude, aberration, valid_mask):
    n = lax.axis_size("tile")
    patterns, acts = hadamard.shape
    subs, samples = amplitude.shape[0], amplitude.shape[1]
    flat = samples * samples
    per_step = math.gcd(subs, 16)
    commands = (stroke[None, :] * hadamard.astype(jnp.float32)).astype(jnp.bfloat16)
    low_slab, up_slab = passed_along(influence[2], "tile", 1), passed_along(influence[0], "tile", -1)
    low_cmds, up_cmds = passed_along(commands, "tile", 1), passed_along(commands, "tile", -1)
    cmds = jnp.stack([low_cmds, commands, up_cmds])
    amp, abe = amplitude.reshape(subs, flat), aberration.reshape(subs, flat)
    real, imag = amp * jnp.cos(abe), amp * jnp.sin(abe)
    mask = valid_mask.astype(jnp.float32)[:, None]
    table = jnp.asarray(dft_table(samples, PIX), dtype=jnp.bfloat16)
    width = per_step * flat
    slopes = pl.pallas_call(
        functools.partial(slopes_kernel, per_step, flat),
        grid=(subs // per_step,),
        out_shape=jax.ShapeDtypeStruct((2, subs, patterns), jnp.bfloat16),
        in_specs=[
            pl.BlockSpec((3, patterns, acts), lambda i: (0, 0, 0)),
            pl.BlockSpec((1, acts, width), lambda i: (1, 0, i)),
            pl.BlockSpec((acts, width), lambda i: (0, i)),
            pl.BlockSpec((acts, width), lambda i: (0, i)),
            pl.BlockSpec((per_step, flat), lambda i: (i, 0)),
            pl.BlockSpec((per_step, flat), lambda i: (i, 0)),
            pl.BlockSpec((per_step, 1), lambda i: (i, 0)),
            pl.BlockSpec((2 * flat, 2 * flat), lambda i: (0, 0)),
        ],
        out_specs=pl.BlockSpec((2, per_step, patterns), lambda i: (0, i, 0)),
        compiler_params=pltpu.CompilerParams(vmem_limit_bytes=40 * 1024 * 1024),
        name="slopes",
    )(cmds, influence, low_slab, up_slab, real, imag, mask, table)
    signs = hadamard.T.astype(jnp.bfloat16)
    summed = pl.pallas_call(
        functools.partial(gather_kernel, n),
        out_shape=jax.ShapeDtypeStruct((2, acts, n * subs), jnp.float32),
        in_specs=[pl.BlockSpec(memory_space=pltpu.VMEM)] * 2,
        out_specs=pl.BlockSpec(memory_space=pltpu.VMEM),
        scratch_shapes=[
            pltpu.VMEM((2, n * subs, patterns), jnp.bfloat16),
            pltpu.SemaphoreType.DMA,
            pltpu.SemaphoreType.DMA((n,)),
            pltpu.SemaphoreType.DMA((n,)),
        ],
        compiler_params=pltpu.CompilerParams(collective_id=0, has_side_effects=True),
        name="gather",
    )(slopes, signs)
    return summed.transpose(1, 0, 2) / (patterns * stroke)[:, None, None]


def solution(mesh):
    placed = (
        P(None, "tile"),
        P(("group", "tile")),
        P(None, ("group", "tile"), None),
        P(("group", "tile"), None, None),
        P(("group", "tile"), None, None),
        P(("group", "tile")),
    )
    return jax.shard_map(
        per_device,
        mesh=mesh,
        in_specs=placed,
        out_specs=P(("group", "tile"), None, None),
        check_vma=False,
    )
```

```python
import functools
import math

import jax
import jax.numpy as jnp
import numpy as np
from jax import lax
from jax.experimental import pallas as pl
from jax.experimental.pallas import tpu as pltpu
from jax.sharding import PartitionSpec as P

PIX = 16
MESH = pl.DeviceIdType.MESH
NT = (((1,), (1,)), ((), ()))


def dft_table(samples, pixels):
    freqs = np.arange(pixels) - pixels / 2.0
    wave = np.exp(-2j * np.pi * freqs[:, None] * np.arange(samples)[None, :] / (2.0 * samples))
    kron = np.kron(wave, wave)
    return np.block([[kron.real, -kron.imag], [kron.imag, kron.real]]).astype(np.float32)


def poly_fit(func, degree):
    fit = np.polynomial.chebyshev.Chebyshev.interpolate(func, degree, domain=[0.0, 0.25])
    return [float(c) for c in fit.convert(kind=np.polynomial.Polynomial).coef]


def sin_over_r(z):
    return 2 * np.pi * np.sinc(2 * np.sqrt(z))


COS = poly_fit(lambda z: np.cos(2 * np.pi * np.sqrt(z)), 5)
SIN = poly_fit(sin_over_r, 5)


def horner(coefs, z):
    total = coefs[-1] * z + coefs[-2]
    for c in coefs[-3::-1]:
        total = total * z + c
    return total


def cos_sin(phase):
    turns = phase * (1.0 / (2.0 * math.pi))
    r = turns - jnp.round(turns)
    z = r * r
    return horner(COS, z), r * horner(SIN, z)


def column_sums(planes):
    pix = len(planes)
    run = planes[-1]
    nested = run
    for plane in planes[-2::-1]:
        run = run + plane
        nested = nested + run
    places = lax.broadcasted_iota(jnp.int32, run.shape, 0).astype(jnp.float32)
    centre = (pix - 1) / 2.0
    along_u = nested - (centre + 1.0) * run
    along_v = run * (places - centre)
    return [jnp.sum(x, axis=0, keepdims=True) for x in (run, along_u, along_v)]


def spot_rows(phase, real, imag, table):
    patterns = phase.shape[0]
    cs, sn = cos_sin(phase)
    even = jnp.concatenate([(cs * real).astype(jnp.bfloat16), (cs * imag).astype(jnp.bfloat16)], axis=1)
    odd = jnp.concatenate([(sn * -imag).astype(jnp.bfloat16), (sn * real).astype(jnp.bfloat16)], axis=1)
    field = jnp.concatenate([even, odd], axis=0)
    focal = lax.dot_general(table, field, NT, preferred_element_type=jnp.float32)
    half = focal.shape[0] // 2
    squares, crosses = [], []
    for u in range(PIX):
        re = focal[u * PIX:(u + 1) * PIX]
        im = focal[half + u * PIX:half + (u + 1) * PIX]
        c_re, s_re = re[:, :patterns], re[:, patterns:]
        c_im, s_im = im[:, :patterns], im[:, patterns:]
        squares.append((c_re * c_re + c_im * c_im) + (s_re * s_re + s_im * s_im))
        crosses.append(c_re * s_re + c_im * s_im)
    p0, pu, pv = column_sums(squares)
    q0, qu, qv = [2.0 * x for x in column_sums(crosses)]
    scale = 1.0 / ((p0 + q0) * (p0 - q0))
    return (qu * p0 - pu * q0) * scale, (qv * p0 - pv * q0) * scale


def diagonal_column(row):
    k = row.shape[1]
    shape = (k, k)
    same = lax.broadcasted_iota(jnp.int32, shape, 0) == lax.broadcasted_iota(jnp.int32, shape, 1)
    return jnp.sum(jnp.where(same, jnp.broadcast_to(row, shape), 0.0), axis=1, keepdims=True)


def commands_of(had, stroke):
    return (stroke * had.astype(jnp.float32).T).astype(jnp.bfloat16)


def slopes_kernel(
    n, chunks, per, flat,
    had_ref, stroke_ref, infl_ref, amp_ref, abe_ref, mask_ref, table_ref,
    out_ref,
    mid_buf, low_buf, up_buf, had_low, had_up, stroke_low, stroke_up, real, imag, rows,
    mid_sems, send_sems, recv_sems, cmd_send, cmd_recv,
):
    me = lax.axis_index("tile")
    has_low, has_up = me > 0, me < n - 1
    low_id, up_id = {"tile": jnp.maximum(me - 1, 0)}, {"tile": jnp.minimum(me + 1, n - 1)}
    width = per * flat
    barrier = pltpu.get_barrier_semaphore()

    @pl.when(has_low)
    def _():
        pl.semaphore_signal(barrier, inc=1, device_id=low_id, device_id_type=MESH)

    @pl.when(has_up)
    def _():
        pl.semaphore_signal(barrier, inc=1, device_id=up_id, device_id_type=MESH)

    def columns(c):
        return pl.ds(pl.multiple_of(c * width, width), width)

    def mid_copy(c):
        return pltpu.make_async_copy(infl_ref.at[1, :, columns(c)], mid_buf.at[c], mid_sems.at[c])

    def remote(src, dst, send, recv, device):
        return pltpu.make_async_remote_copy(
            src_ref=src, dst_ref=dst, send_sem=send, recv_sem=recv, device_id=device, device_id_type=MESH
        )

    def to_up(c):
        return remote(infl_ref.at[2, :, columns(c)], low_buf.at[c], send_sems.at[0, c], recv_sems.at[0, c], up_id)

    def to_low(c):
        return remote(infl_ref.at[0, :, columns(c)], up_buf.at[c], send_sems.at[1, c], recv_sems.at[1, c], low_id)

    def cmds_up():
        return (
            remote(had_ref, had_low, cmd_send.at[0], cmd_recv.at[0], up_id),
            remote(stroke_ref, stroke_low, cmd_send.at[1], cmd_recv.at[1], up_id),
        )

    def cmds_low():
        return (
            remote(had_ref, had_up, cmd_send.at[2], cmd_recv.at[2], low_id),
            remote(stroke_ref, stroke_up, cmd_send.at[3], cmd_recv.at[3], low_id),
        )

    inner = jnp.logical_and(has_low, has_up)

    @pl.when(inner)
    def _():
        pl.semaphore_wait(barrier, 2)

    @pl.when(jnp.logical_not(inner))
    def _():
        pl.semaphore_wait(barrier, 1)

    @pl.when(has_up)
    def _():
        for copy in cmds_up():
            copy.start()

    @pl.when(has_low)
    def _():
        for copy in cmds_low():
            copy.start()

    @pl.loop(0, chunks)
    def _(c):
        @pl.when(has_up)
        def _():
            to_up(c).start()

        @pl.when(has_low)
        def _():
            to_low(c).start()

        mid_copy(c).start()

    @pl.when(jnp.logical_not(has_low))
    def _():
        had_low[...] = jnp.zeros_like(had_low)
        stroke_low[...] = jnp.zeros_like(stroke_low)
        low_buf[...] = jnp.zeros_like(low_buf)

    @pl.when(jnp.logical_not(has_up))
    def _():
        had_up[...] = jnp.zeros_like(had_up)
        stroke_up[...] = jnp.zeros_like(stroke_up)
        up_buf[...] = jnp.zeros_like(up_buf)

    cs, sn = cos_sin(abe_ref[...])
    whole_real, whole_imag = (amp_ref[...] * cs).T, (amp_ref[...] * sn).T
    for c in range(chunks):
        real[c] = whole_real[c * per:(c + 1) * per]
        imag[c] = whole_imag[c * per:(c + 1) * per]

    @pl.when(has_up)
    def _():
        for copy in cmds_up():
            copy.wait_send()
        for copy in cmds_low():
            copy.wait_recv()

    @pl.when(has_low)
    def _():
        for copy in cmds_low():
            copy.wait_send()
        for copy in cmds_up():
            copy.wait_recv()

    mid_cmds = commands_of(had_ref[...], stroke_ref[...])
    low_cmds = commands_of(had_low[...], stroke_low[...])
    up_cmds = commands_of(had_up[...], stroke_up[...])

    @pl.loop(0, chunks)
    def _(c):
        mid_copy(c).wait()

        @pl.when(has_low)
        def _():
            to_up(c).wait_recv()

        @pl.when(has_up)
        def _():
            to_low(c).wait_recv()

        rows_u, rows_v = [], []
        for k in range(per):
            cols = slice(k * flat, (k + 1) * flat)
            phase = jnp.dot(low_cmds, low_buf[c, :, cols], preferred_element_type=jnp.float32)
            phase += jnp.dot(mid_cmds, mid_buf[c, :, cols], preferred_element_type=jnp.float32)
            phase += jnp.dot(up_cmds, up_buf[c, :, cols], preferred_element_type=jnp.float32)
            along_u, along_v = spot_rows(phase, real[c, k:k + 1, :], imag[c, k:k + 1, :], table_ref[...])
            rows_u.append(along_u)
            rows_v.append(along_v)
        rows[c, 0] = jnp.concatenate(rows_u, axis=0)
        rows[c, 1] = jnp.concatenate(rows_v, axis=0)

    mask = diagonal_column(mask_ref[...].astype(jnp.float32))
    for j in range(2):
        whole = jnp.concatenate([rows[c, j] for c in range(chunks)], axis=0)
        out_ref[j] = (whole * mask).astype(out_ref.dtype)

    @pl.loop(0, chunks)
    def _(c):
        @pl.when(has_up)
        def _():
            to_up(c).wait_send()

        @pl.when(has_low)
        def _():
            to_low(c).wait_send()


def gather_kernel(n, mine_ref, had_ref, stroke_ref, out_ref, held, own_sem, send_sems, recv_sems):
    me = lax.axis_index("tile")
    subs = mine_ref.shape[1]
    barrier = pltpu.get_barrier_semaphore()

    @pl.loop(1, n)
    def _(k):
        pl.semaphore_signal(barrier, inc=1, device_id={"tile": lax.rem(me + k, n)}, device_id_type=MESH)

    pl.semaphore_wait(barrier, n - 1)
    slot = held.at[:, pl.ds(pl.multiple_of(me * subs, subs), subs), :]
    own = pltpu.make_async_copy(mine_ref, slot, own_sem)
    own.start()

    def push(k):
        return pltpu.make_async_remote_copy(
            src_ref=mine_ref,
            dst_ref=slot,
            send_sem=send_sems.at[k],
            recv_sem=recv_sems.at[k],
            device_id={"tile": lax.rem(me + k, n)},
            device_id_type=MESH,
        )

    @pl.loop(1, n)
    def _(k):
        push(k).start()

    patterns = had_ref.shape[1]
    signs = had_ref[...].astype(jnp.float32).astype(jnp.bfloat16)
    scale = patterns * diagonal_column(stroke_ref[...])
    own.wait()

    @pl.loop(1, n)
    def _(k):
        push(k).wait()

    for c in range(2):
        summed = lax.dot_general(signs, held[c], NT, preferred_element_type=jnp.float32)
        out_ref[:, c, :] = summed / scale


def per_device(hadamard, stroke, influence, amplitude, aberration, valid_mask):
    n = lax.axis_size("tile")
    patterns, acts = hadamard.shape
    subs, samples = amplitude.shape[0], amplitude.shape[1]
    flat = samples * samples
    per = math.gcd(subs, 4)
    chunks = subs // per
    had = hadamard.T
    amp = amplitude.transpose(1, 2, 0).reshape(flat, subs)
    abe = aberration.transpose(1, 2, 0).reshape(flat, subs)
    stroke = stroke.reshape(1, acts)
    mask = valid_mask.reshape(1, subs)
    table = jnp.asarray(dft_table(samples, PIX), dtype=jnp.bfloat16)
    vmem = pl.BlockSpec(memory_space=pltpu.VMEM)
    slab = pltpu.VMEM((chunks, acts, per * flat), jnp.bfloat16)
    slopes = pl.pallas_call(
        functools.partial(slopes_kernel, n, chunks, per, flat),
        out_shape=jax.ShapeDtypeStruct((2, subs, patterns), jnp.bfloat16),
        in_specs=[vmem, vmem, pl.BlockSpec(memory_space=pltpu.HBM), vmem, vmem, vmem, vmem],
        out_specs=vmem,
        scratch_shapes=[
            slab, slab, slab,
            pltpu.VMEM((acts, patterns), jnp.int32),
            pltpu.VMEM((acts, patterns), jnp.int32),
            pltpu.VMEM((1, acts), jnp.float32),
            pltpu.VMEM((1, acts), jnp.float32),
            pltpu.VMEM((chunks, per, flat), jnp.float32),
            pltpu.VMEM((chunks, per, flat), jnp.float32),
            pltpu.VMEM((chunks, 2, per, patterns), jnp.float32),
            pltpu.SemaphoreType.DMA((chunks,)),
            pltpu.SemaphoreType.DMA((2, chunks)),
            pltpu.SemaphoreType.DMA((2, chunks)),
            pltpu.SemaphoreType.DMA((4,)),
            pltpu.SemaphoreType.DMA((4,)),
        ],
        compiler_params=pltpu.CompilerParams(
            collective_id=1, has_side_effects=True, vmem_limit_bytes=40 * 1024 * 1024
        ),
        name="slopes",
    )(had, stroke, influence, amp, abe, mask, table)
    return pl.pallas_call(
        functools.partial(gather_kernel, n),
        out_shape=jax.ShapeDtypeStruct((acts, 2, n * subs), jnp.float32),
        in_specs=[vmem] * 3,
        out_specs=vmem,
        scratch_shapes=[
            pltpu.VMEM((2, n * subs, patterns), jnp.bfloat16),
            pltpu.SemaphoreType.DMA,
            pltpu.SemaphoreType.DMA((n,)),
            pltpu.SemaphoreType.DMA((n,)),
        ],
        compiler_params=pltpu.CompilerParams(collective_id=0, has_side_effects=True),
        name="gather",
    )(slopes, had, stroke)


def solution(mesh):
    placed = (
        P(None, "tile"),
        P(("group", "tile")),
        P(None, ("group", "tile"), None),
        P(("group", "tile"), None, None),
        P(("group", "tile"), None, None),
        P(("group", "tile")),
    )
    return jax.shard_map(
        per_device,
        mesh=mesh,
        in_specs=placed,
        out_specs=P(("group", "tile"), None, None),
        check_vma=False,
    )
```
